512 devices in a mesh: dp: 8 (over y, core), expert: 64 (over z, x).
Axes of the slice: x: 4, y: 4, z: 16, core: 2. Of those that a mesh axis runs over, the one named last changes fastest.
Arguments:
- tokens: bfloat16 [65536, 1920], P(('dp', 'expert')), may hold values from -10 to 10
- assignment: int32 [65536], P(('dp', 'expert')), may hold values from 0 to 63, as said below
- centroids: bfloat16 [64, 1920], P('expert'), may hold values from -0.125 to 0.125
- norm_gain: float32 [64, 1920], P('expert'), may hold values from 0.25 to 1.75
- inner_weight: bfloat16 [64, 4096, 1920], P('expert', 'dp'), may hold values from -0.125 to 0.125
- outer_weight: bfloat16 [64, 4096, 1920], P('expert', 'dp'), may hold values from -0.09375 to 0.09375
Outputs:
- layer_out: bfloat16 [65536, 1920], P(('dp', 'expert'))
The draws below stay inside these ranges and needn't reach their ends.
Inputs may be any that keep to these rules, and one draw needn't show every extreme that they name: `assignment`: each expert is assigned exactly 128 of the tokens of the devices that share one index of dp. One device assigns at most 4 of its tokens to one expert, and every expert gets exactly 4 tokens from some device of each index of dp.
All inputs are finite; a program needn't handle non-finite values.
Results may differ from the reference program's by a relative error of at most 0.007.
Values may be sent and summed in bfloat16 or wider, within the bound.
A program may use at most 64 MiB of HBM per device.

```python
import jax
import jax.numpy as jnp
from jax import lax

D = 1920
FF = 4096
TOK_DEV = 128
EXPERTS = 64
CAP = 4
TOKENS = 65536
N_DP = 8
N_EXPERT = 64


def draw_tokens(key, part):
    normal_key = jax.random.fold_in(key, 0)
    values = jax.random.normal(normal_key, (TOKENS, D), jnp.float32)
    return jnp.clip(values, -10.0, 10.0).astype(jnp.bfloat16)


def draw_assignment(key, part):

    def one_row(row_key):
        pool_key, source_key, expert_key, order_key = jax.random.split(row_key, 4)
        pool = jnp.repeat(jnp.arange(1, EXPERTS, dtype=jnp.int32), CAP)
        picked = jax.random.permutation(pool_key, pool)[:TOK_DEV - CAP]
        offsets_row = jnp.concatenate([jnp.zeros((CAP,), jnp.int32), picked])
        shift_perm = jax.random.permutation(source_key, N_EXPERT).astype(jnp.int32)
        relabel = jax.random.permutation(expert_key, EXPERTS).astype(jnp.int32)

        def one_source(source_index):
            token_order = jax.random.permutation(jax.random.fold_in(order_key, source_index), TOK_DEV)
            return relabel[(shift_perm[source_index] + offsets_row[token_order]) % EXPERTS]
        return jax.vmap(one_source)(jnp.arange(N_EXPERT, dtype=jnp.int32))
    row_keys = jax.vmap(lambda index: jax.random.fold_in(key, index))(jnp.arange(N_DP, dtype=jnp.int32))
    table = jax.vmap(one_row)(row_keys)
    return table.reshape(-1).astype(jnp.int32)


def level_of(own_key, extent, shards, least, largest):
    def one(position, parts):
        heights = jax.random.uniform(jax.random.fold_in(jax.random.fold_in(own_key, 6), position), (parts,), jnp.float32, least / len(shards), largest / len(shards))
        return jnp.repeat(jnp.exp(heights), extent[position] // parts).reshape((-1,) + (1,) * (len(extent) - position - 1))

    gain = one(*shards[0])
    for cut in shards[1:]:
        gain = gain * one(*cut)
    return gain


def normal_values(stream_key, dims, deviation, limit, cuts=(), kind=jnp.bfloat16):
    loudness = level_of(stream_key, dims, cuts, -0.22, 0.18) if cuts else 1.0
    result = jax.random.normal(stream_key, dims, jnp.float32) * deviation * loudness
    return jnp.minimum(jnp.maximum(result, -limit), limit).astype(kind)


def setup_inputs(seed: int = 0) -> dict:
    arg_keys = jax.random.split(jax.random.key(seed), 7)
    tokens = draw_tokens(jax.random.fold_in(arg_keys[6], 71), 0)
    assignment = draw_assignment(jax.random.fold_in(arg_keys[6], 71), 0)
    centroids = normal_values(arg_keys[2], (EXPERTS, D), D ** -0.5, 0.125, ((0, 64),))
    norm_gain = jnp.clip(1.0 + 0.15 * jax.random.normal(arg_keys[3], (EXPERTS, D), jnp.float32), 0.25, 1.75)
    inner_weight = normal_values(arg_keys[4], (EXPERTS, FF, D), D ** -0.5, 0.125, ((0, 64), (1, 8)))
    outer_weight = normal_values(arg_keys[5], (EXPERTS, FF, D), FF ** -0.5, 0.09375, ((0, 64), (1, 8)))
    return dict(tokens=tokens, assignment=assignment, centroids=centroids, norm_gain=norm_gain, inner_weight=inner_weight, outer_weight=outer_weight)


epsilon = 1e-05

def normalize(rows_in, gain_row):
    values = rows_in.astype(jnp.float32)
    center = lax.optimization_barrier(jnp.mean(values, axis=1, keepdims=True))
    spread = lax.optimization_barrier(jnp.mean(jnp.square(values - center), axis=1, keepdims=True))
    return ((values - center) * lax.rsqrt(spread + epsilon) * gain_row).astype(jnp.bfloat16)

def reference(tokens, assignment, centroids, norm_gain, inner_weight, outer_weight):
    per_expert = TOK_DEV * N_DP
    share = FF // N_DP
    order = jnp.argsort(assignment, stable=True).astype(jnp.int32)
    grouped = order.reshape(EXPERTS, per_expert)

    def one_expert(operands):
        index_rows, gain_row, inner_mat, outer_mat = operands
        normed = normalize(jnp.take(tokens, index_rows, axis=0), gain_row[None, :])
        inner_act = lax.dot_general(normed, inner_mat, (((1,), (1,)), ((), ())), preferred_element_type=jnp.float32)
        hidden = jnp.maximum(inner_act, 0.0).astype(jnp.bfloat16)
        total = jnp.zeros((per_expert, D), jnp.float32)
        for group in range(N_DP):
            part_sum = jnp.dot(hidden[:, group * share:(group + 1) * share], outer_mat[group * share:(group + 1) * share], preferred_element_type=jnp.float32)
            rounded = lax.optimization_barrier(part_sum.astype(jnp.bfloat16))
            total = total + rounded.astype(jnp.float32)
        return total.astype(jnp.bfloat16)
    outputs = lax.map(one_expert, (grouped, norm_gain, inner_weight, outer_weight))
    expert_out = jnp.zeros((EXPERTS * per_expert, D), jnp.bfloat16).at[grouped.reshape(-1)].set(outputs.reshape(-1, D))
    scores = jnp.dot(tokens, centroids.T, preferred_element_type=jnp.float32)
    chosen = jnp.take_along_axis(scores, assignment[:, None], axis=1)[:, 0]
    gate_value = jax.nn.sigmoid(chosen).astype(jnp.bfloat16)
    mixed_out = tokens.astype(jnp.float32) + gate_value.astype(jnp.float32)[:, None] * expert_out.astype(jnp.float32)
    return mixed_out.astype(jnp.bfloat16)
```

```python
import functools

import jax
import jax.numpy as jnp
from jax import lax
from jax.experimental import pallas as pl
from jax.experimental.pallas import tpu as pltpu
from jax.sharding import PartitionSpec as P

MESH = pl.DeviceIdType.MESH
EPS = 1e-05
NZ, NX, NY = 16, 4, 4
CAP = 4
CHUNKS = ((1, 15, 7, 9), (2, 14, 6, 10), (3, 13, 5, 11), (4, 12, 8, 0))
NCH = len(CHUNKS)
PER = 16
XS = (1, 2, 3, 0)
OFFS = tuple((dz, dx) for c in CHUNKS for dz in c for dx in XS)
ROWS = PER * CAP
F32, BF16 = jnp.float32, jnp.bfloat16


def kernel(
    tok_hbm, asg_ref, cen_ref, gain_ref, w1_hbm, w2_hbm, out_ref,
    tok, w1, w2, snd, rcv, grp, psend, precv, part, qs, rq, ret, back, gates,
    lsem, dsend, drecv, asend, arecv, psem_s, psem_r, qsem_s, qsem_r, rsend, rrecv,
):
    dp, e = lax.axis_index("dp"), lax.axis_index("expert")
    y, c = dp // 2, lax.rem(dp, 2)
    z, x = e // NX, lax.rem(e, NX)
    d_model = tok.shape[1]

    tok_cp = pltpu.make_async_copy(tok_hbm, tok, lsem.at[0])
    w1_cp = pltpu.make_async_copy(w1_hbm.at[0], w1, lsem.at[1])
    w2_cp = pltpu.make_async_copy(w2_hbm.at[0], w2, lsem.at[2])
    tok_cp.start()
    w1_cp.start()
    w2_cp.start()

    def chip(step):
        return lax.rem(y + step, NY) * 2 + c

    partner = (y * 2 + (1 - c), e)
    dirf = 1 + 2 * c
    dirb = 3 - 2 * c
    ahead, behind = (chip(dirf), e), (chip(dirb), e)

    def to(dz, dx):
        return (dp, lax.rem(z + dz, NZ) * NX + lax.rem(x + dx, NX))

    bar = pltpu.get_barrier_semaphore()
    peers = [to(dz, dx) for dz, dx in OFFS[:-1]] + [partner, ahead, behind]
    for peer in peers:
        pl.semaphore_signal(bar, inc=1, device_id=peer, device_id_type=MESH)

    n_tok = tok.shape[0]
    a_row = asg_ref[...]
    ri = lax.broadcasted_iota(jnp.int32, (n_tok, n_tok), 0)
    ci = lax.broadcasted_iota(jnp.int32, (n_tok, n_tok), 1)
    a_lane = jnp.broadcast_to(a_row, (n_tok, n_tok))
    a_col = jnp.sum(jnp.where(ri == ci, a_lane, 0), axis=1, keepdims=True)
    same = a_lane == a_col
    pos_row = jnp.sum(jnp.where(same & (ri < ci), 1, 0), axis=0, keepdims=True)
    pos_col = jnp.sum(jnp.where(same & (ci < ri), 1, 0), axis=1, keepdims=True)

    def row_of(a, pos):
        dz = (a // NX - z + NZ) & (NZ - 1)
        dx = (a - z * NX - x + NZ * NX) & (NX - 1)
        kz = jnp.zeros_like(a)
        for i, v in enumerate(v for ch in CHUNKS for v in ch):
            kz = jnp.where(dz == v, i, kz)
        kx = (dx + NX - 1) & (NX - 1)
        return (kz * NX + kx) * CAP + pos


    row_r = row_of(a_row, pos_row)
    row_c = row_of(a_col, pos_col)
    n_slot = NCH * ROWS
    pick = jnp.where(
        lax.broadcasted_iota(jnp.int32, (n_slot, n_tok), 0) == row_r, 1.0, 0.0
    ).astype(BF16)
    tok_cp.wait()
    slots = jnp.dot(pick, tok[...], preferred_element_type=F32)
    snd[...] = slots.reshape(NCH * PER, CAP, d_model).astype(BF16)

    pl.semaphore_wait(bar, len(peers))

    def dispatch(k):
        return pltpu.make_async_remote_copy(
            src_ref=snd.at[k],
            dst_ref=rcv.at[k],
            send_sem=dsend,
            recv_sem=drecv.at[k // PER],
            device_id=to(*OFFS[k]),
            device_id_type=MESH,
        )

    last = NCH * PER - 1
    for k in range(last):
        dispatch(k).start()
    own_in = pltpu.make_async_copy(snd.at[last], rcv.at[last], lsem.at[3])
    own_in.start()

    def all_of(ref, first, count, sem):
        view = ref.at[pl.ds(first, count)]
        return pltpu.make_async_copy(view, view, sem)

    def n_remote(j):
        return PER - 1 if j == NCH - 1 else PER

    def block(j, s, r):
        return grp.at[j, pl.ds((s * NY + r) * ROWS, ROWS)]

    def remote(src, dst, ssem, rsem, dev):
        return pltpu.make_async_remote_copy(
            src_ref=src, dst_ref=dst, send_sem=ssem, recv_sem=rsem,
            device_id=dev, device_id_type=MESH,
        )

    rf, rb = 1 + 2 * c, 3 - 2 * c

    def ag_ahead(j):
        return remote(block(j, 0, 0), block(j, 0, rf), asend.at[j, 0], arecv.at[j, rf], ahead)

    def ag_behind(j):
        return remote(block(j, 0, 0), block(j, 0, rb), asend.at[j, 1], arecv.at[j, rb], behind)

    def ag_on(j):
        return remote(block(j, 0, rf), block(j, 0, 2), asend.at[j, 2], arecv.at[j, 2], ahead)

    def ag_side(j, r):
        return remote(
            block(j, 0, r), block(j, 1, r), asend.at[j, 4 + r], arecv.at[j, NY + r], partner
        )

    def arrived(j, s, r):
        view = block(j, s, r)
        pltpu.make_async_copy(view, view, arecv.at[j, s * NY + r]).wait()

    def stage_a(j):
        all_of(rcv, j * PER, n_remote(j), drecv.at[j]).wait()
        if j == NCH - 1:
            own_in.wait()
        v = rcv[pl.ds(j * PER, PER)].astype(F32).reshape(ROWS, d_model)
        center = jnp.mean(v, axis=1, keepdims=True)
        dev = v - center
        spread = jnp.mean(dev * dev, axis=1, keepdims=True)
        normed = (dev * lax.rsqrt(spread + EPS) * gain_ref[...]).astype(BF16)
        grp[j, pl.ds(0, ROWS)] = normed
        ag_ahead(j).start()
        ag_behind(j).start()
        ag_side(j, 0).start()
        score = jnp.sum(v * cen_ref[...].astype(F32), axis=1, keepdims=True)
        gate = (1.0 / (1.0 + jnp.exp(-score))).astype(BF16).astype(F32)
        gates[j] = jnp.broadcast_to(gate, (ROWS, 128))

    def stage_b(j):
        arrived(j, 0, rf)
        ag_on(j).start()
        arrived(j, 0, rb)
        ag_side(j, 1).start()
        ag_side(j, 3).start()

    def stage_c(j):
        arrived(j, 0, 2)
        ag_side(j, 2).start()

    def mlp(rows):
        act = lax.dot_general(
            rows, w1[...], (((1,), (1,)), ((), ())), preferred_element_type=F32
        )
        hidden = jnp.maximum(act, 0.0).astype(BF16)
        return jnp.dot(hidden, w2[...], preferred_element_type=F32)

    half = NY * ROWS

    def swap(j):
        return remote(psend.at[j], precv.at[j], psem_s.at[j], psem_r.at[j], partner)

    def stage_d(j):
        if j == 0:
            w1_cp.wait()
            w2_cp.wait()
        for r in range(NY):
            arrived(j, 1, r)
        psend[j] = mlp(grp[j, pl.ds(half, half)]).astype(BF16)
        swap(j).start()
        part[j % 2] = mlp(grp[j, pl.ds(0, half)])

    rc, rd = 3 - 2 * c, 1 + 2 * c

    def q_far(j):
        return remote(qs.at[j, 0], rq.at[j, 0], qsem_s.at[j, 0], qsem_r.at[j, 0], ahead)

    def q_on(j):
        return remote(qs.at[j, 1], rq.at[j, 1], qsem_s.at[j, 1], qsem_r.at[j, 1], ahead)

    def q_near(j):
        return remote(qs.at[j, 2], rq.at[j, 2], qsem_s.at[j, 2], qsem_r.at[j, 2], behind)

    def q_wait(j, i):
        view = rq.at[j, i]
        pltpu.make_async_copy(view, view, qsem_r.at[j, i]).wait()

    def rows_of(r):
        return pl.ds(pl.multiple_of(r * ROWS, ROWS), ROWS)

    def pair_sum(j, r):
        return part[j % 2, rows_of(r)] + precv[j, rows_of(r)].astype(F32)

    def stage_e(j):
        view = precv.at[j]
        pltpu.make_async_copy(view, view, psem_r.at[j]).wait()
        qs[j, 0] = pair_sum(j, 2).astype(BF16)
        q_far(j).start()
        qs[j, 2] = pair_sum(j, rd).astype(BF16)
        q_near(j).start()

    def stage_f(j):
        q_wait(j, 0)
        qs[j, 1] = (pair_sum(j, rc) + rq[j, 0].astype(F32)).astype(BF16)
        q_on(j).start()

    def give_back(k):
        dz, dx = OFFS[k]
        return pltpu.make_async_remote_copy(
            src_ref=ret.at[k],
            dst_ref=back.at[k],
            send_sem=rsend,
            recv_sem=rrecv.at[k // PER],
            device_id=to(NZ - dz, NX - dx),
            device_id_type=MESH,
        )

    own_out = pltpu.make_async_copy(ret.at[last], back.at[last], lsem.at[4])

    def stage_g(j):
        q_wait(j, 2)
        total = pair_sum(j, 0) + rq[j, 2].astype(F32)
        q_wait(j, 1)
        total = total + rq[j, 1].astype(F32)
        scaled = total * gates[j][:, :1]
        ret[pl.ds(j * PER, PER)] = scaled.reshape(PER, CAP, d_model).astype(BF16)
        for k in range(j * PER, j * PER + n_remote(j)):
            give_back(k).start()
        if j == NCH - 1:
            own_out.start()

    for t in range(NCH + 2):
        for stage, j in (
            (stage_a, t), (stage_c, t - 1), (stage_f, t - 2), (stage_d, t - 1),
            (stage_g, t - 2), (stage_b, t), (stage_e, t - 1),
        ):
            if 0 <= j < NCH:
                stage(j)

    acc = tok[...].astype(F32)
    for j in range(NCH):
        all_of(back, j * PER, n_remote(j), rrecv.at[j]).wait()
        if j == NCH - 1:
            own_out.wait()
        rows = back[pl.ds(j * PER, PER)].astype(F32).reshape(ROWS, d_model).astype(BF16)
        choose = jnp.where(
            lax.broadcasted_iota(jnp.int32, (n_tok, ROWS), 1) + j * ROWS == row_c, 1.0, 0.0
        ).astype(BF16)
        acc = acc + jnp.dot(choose, rows, preferred_element_type=F32)
    out_ref[...] = acc.astype(BF16)

    all_of(snd, 0, last, dsend).wait()
    all_of(ret, 0, last, rsend).wait()
    for j in range(NCH):
        ag_ahead(j).wait_send()
        ag_behind(j).wait_send()
        ag_on(j).wait_send()
        for r in range(NY):
            ag_side(j, r).wait_send()
        swap(j).wait_send()
        q_far(j).wait_send()
        q_on(j).wait_send()
        q_near(j).wait_send()


def body(tokens, assignment, centroids, norm_gain, inner_weight, outer_weight):
    n_tok, d = tokens.shape
    hidden = inner_weight.shape[1]
    half = NY * ROWS
    vmem, anyspace = pltpu.VMEM, pl.ANY
    dma = pltpu.SemaphoreType.DMA
    return pl.pallas_call(
        kernel,
        out_shape=jax.ShapeDtypeStruct((n_tok, d), BF16),
        in_specs=[
            pl.BlockSpec(memory_space=anyspace),
            pl.BlockSpec(memory_space=vmem),
            pl.BlockSpec(memory_space=vmem),
            pl.BlockSpec(memory_space=vmem),
            pl.BlockSpec(memory_space=anyspace),
            pl.BlockSpec(memory_space=anyspace),
        ],
        out_specs=pl.BlockSpec(memory_space=vmem),
        scratch_shapes=[
            vmem((n_tok, d), BF16),
            vmem((hidden, d), BF16),
            vmem((hidden, d), BF16),
            vmem((NCH * PER, CAP, d), BF16),
            vmem((NCH * PER, CAP, d), BF16),
            vmem((NCH, 2 * half, d), BF16),
            vmem((NCH, half, d), BF16),
            vmem((NCH, half, d), BF16),
            vmem((2, half, d), F32),
            vmem((NCH, 3, ROWS, d), BF16),
            vmem((NCH, 3, ROWS, d), BF16),
            vmem((NCH * PER, CAP, d), BF16),
            vmem((NCH * PER, CAP, d), BF16),
            vmem((NCH, ROWS, 128), F32),
            dma((5,)),
            dma,
            dma((NCH,)),
            dma((NCH, 8)),
            dma((NCH, 8)),
            dma((NCH,)),
            dma((NCH,)),
            dma((NCH, 3)),
            dma((NCH, 3)),
            dma,
            dma((NCH,)),
        ],
        compiler_params=pltpu.CompilerParams(
            collective_id=0, has_side_effects=True, vmem_limit_bytes=60 * 2**20
        ),
    )(tokens, assignment.reshape(1, n_tok), centroids, norm_gain, inner_weight, outer_weight)


def solution(mesh):
    in_specs = (
        P(("dp", "expert"), None),
        P(("dp", "expert")),
        P("expert", None),
        P("expert", None),
        P("expert", "dp", None),
        P("expert", "dp", None),
    )
    out_specs = P(("dp", "expert"), None)
    return jax.shard_map(body, mesh=mesh, in_specs=in_specs, out_specs=out_specs, check_vma=False)
```

```python
import functools

import jax
import jax.numpy as jnp
from jax import lax
from jax.experimental import pallas as pl
from jax.experimental.pallas import tpu as pltpu
from jax.sharding import PartitionSpec as P

MESH = pl.DeviceIdType.MESH
EPS = 1e-05
NZ, NX, NY = 16, 4, 4
CAP = 4
CHUNKS = ((1, 15), (3, 13), (5, 11), (7, 9), (6, 10), (4, 12), (2, 14), (8, 0))
NCH = len(CHUNKS)
PER = NX * len(CHUNKS[0])
LAGS = dict(a=0.0, b=0.9, c=1.6, d=2.3, e=3.2, f=4.0, g=4.9)
NPART = 5
XS = (1, 2, 3, 0)
OFFS = tuple((dz, dx) for c in CHUNKS for dz in c for dx in XS)
ROWS = PER * CAP
F32, BF16 = jnp.float32, jnp.bfloat16


def kernel(
    tok_hbm, asg_ref, cen_ref, gain_ref, w1_hbm, w2_hbm, out_ref,
    tok, w1, w2, snd, rcv, grp, psend, precv, part, qs, rq, ret, back, gates,
    lsem, dsend, drecv, asend, arecv, psem_s, psem_r, qsem_s, qsem_r, rsend, rrecv,
):
    dp, e = lax.axis_index("dp"), lax.axis_index("expert")
    y, c = dp // 2, lax.rem(dp, 2)
    z, x = e // NX, lax.rem(e, NX)
    d_model = tok.shape[1]

    tok_cp = pltpu.make_async_copy(tok_hbm, tok, lsem.at[0])
    w1_cp = pltpu.make_async_copy(w1_hbm.at[0], w1, lsem.at[1])
    w2_cp = pltpu.make_async_copy(w2_hbm.at[0], w2, lsem.at[2])
    tok_cp.start()
    w1_cp.start()
    w2_cp.start()

    def chip(step):
        return lax.rem(y + step, NY) * 2 + c

    partner = (y * 2 + (1 - c), e)
    dirf = 1 + 2 * c
    dirb = 3 - 2 * c
    ahead, behind = (chip(dirf), e), (chip(dirb), e)

    def to(dz, dx):
        return (dp, lax.rem(z + dz, NZ) * NX + lax.rem(x + dx, NX))

    bar = pltpu.get_barrier_semaphore()
    peers = [to(dz, dx) for dz, dx in OFFS[:-1]] + [partner, ahead, behind]
    for peer in peers:
        pl.semaphore_signal(bar, inc=1, device_id=peer, device_id_type=MESH)

    n_tok = tok.shape[0]
    a_row = asg_ref[...]
    ri = lax.broadcasted_iota(jnp.int32, (n_tok, n_tok), 0)
    ci = lax.broadcasted_iota(jnp.int32, (n_tok, n_tok), 1)
    a_lane = jnp.broadcast_to(a_row, (n_tok, n_tok))
    a_col = jnp.sum(jnp.where(ri == ci, a_lane, 0), axis=1, keepdims=True)
    same = a_lane == a_col
    pos_row = jnp.sum(jnp.where(same & (ri < ci), 1, 0), axis=0, keepdims=True)
    pos_col = jnp.sum(jnp.where(same & (ci < ri), 1, 0), axis=1, keepdims=True)

    def row_of(a, pos):
        dz = (a // NX - z + NZ) & (NZ - 1)
        dx = (a - z * NX - x + NZ * NX) & (NX - 1)
        kz = jnp.zeros_like(a)
        for i, v in enumerate(v for ch in CHUNKS for v in ch):
            kz = jnp.where(dz == v, i, kz)
        kx = (dx + NX - 1) & (NX - 1)
        return (kz * NX + kx) * CAP + pos


    row_r = row_of(a_row, pos_row)
    row_c = row_of(a_col, pos_col)
    n_slot = NCH * ROWS
    pick = jnp.where(
        lax.broadcasted_iota(jnp.int32, (n_slot, n_tok), 0) == row_r, 1.0, 0.0
    ).astype(BF16)
    tok_cp.wait()
    slots = jnp.dot(pick, tok[...], preferred_element_type=F32)
    snd[...] = slots.reshape(NCH * PER, CAP, d_model).astype(BF16)

    pl.semaphore_wait(bar, len(peers))

    def dispatch(k):
        return pltpu.make_async_remote_copy(
            src_ref=snd.at[k],
            dst_ref=rcv.at[k],
            send_sem=dsend,
            recv_sem=drecv.at[k // PER],
            device_id=to(*OFFS[k]),
            device_id_type=MESH,
        )

    last = NCH * PER - 1
    for k in range(last):
        dispatch(k).start()
    own_in = pltpu.make_async_copy(snd.at[last], rcv.at[last], lsem.at[3])
    own_in.start()

    def all_of(ref, first, count, sem):
        view = ref.at[pl.ds(first, count)]
        return pltpu.make_async_copy(view, view, sem)

    def n_remote(j):
        return PER - 1 if j == NCH - 1 else PER

    def block(j, s, r):
        return grp.at[j, pl.ds((s * NY + r) * ROWS, ROWS)]

    def remote(src, dst, ssem, rsem, dev):
        return pltpu.make_async_remote_copy(
            src_ref=src, dst_ref=dst, send_sem=ssem, recv_sem=rsem,
            device_id=dev, device_id_type=MESH,
        )

    rf, rb = 1 + 2 * c, 3 - 2 * c

    def ag_ahead(j):
        return remote(block(j, 0, 0), block(j, 0, rf), asend.at[j, 0], arecv.at[j, rf], ahead)

    def ag_behind(j):
        return remote(block(j, 0, 0), block(j, 0, rb), asend.at[j, 1], arecv.at[j, rb], behind)

    def ag_on(j):
        return remote(block(j, 0, rf), block(j, 0, 2), asend.at[j, 2], arecv.at[j, 2], ahead)

    def ag_side(j, r):
        return remote(
            block(j, 0, r), block(j, 1, r), asend.at[j, 4 + r], arecv.at[j, NY + r], partner
        )

    def arrived(j, s, r):
        view = block(j, s, r)
        pltpu.make_async_copy(view, view, arecv.at[j, s * NY + r]).wait()

    def stage_a(j):
        all_of(rcv, j * PER, n_remote(j), drecv.at[j]).wait()
        if j == NCH - 1:
            own_in.wait()
        v = rcv[pl.ds(j * PER, PER)].astype(F32).reshape(ROWS, d_model)
        center = jnp.mean(v, axis=1, keepdims=True)
        dev = v - center
        spread = jnp.mean(dev * dev, axis=1, keepdims=True)
        normed = (dev * lax.rsqrt(spread + EPS) * gain_ref[...]).astype(BF16)
        grp[j, pl.ds(0, ROWS)] = normed
        ag_ahead(j).start()
        ag_behind(j).start()
        ag_side(j, 0).start()
        score = jnp.sum(v * cen_ref[...].astype(F32), axis=1, keepdims=True)
        gate = (1.0 / (1.0 + jnp.exp(-score))).astype(BF16).astype(F32)
        gates[j] = jnp.broadcast_to(gate, (ROWS, 128))

    def stage_b(j):
        arrived(j, 0, rf)
        ag_on(j).start()
        arrived(j, 0, rb)
        ag_side(j, 1).start()
        ag_side(j, 3).start()

    def stage_c(j):
        arrived(j, 0, 2)
        ag_side(j, 2).start()

    def mlp(rows):
        act = lax.dot_general(
            rows, w1[...], (((1,), (1,)), ((), ())), preferred_element_type=F32
        )
        hidden = jnp.maximum(act, 0.0).astype(BF16)
        return jnp.dot(hidden, w2[...], preferred_element_type=F32)

    half = NY * ROWS

    def swap(j):
        return remote(psend.at[j], precv.at[j], psem_s.at[j], psem_r.at[j], partner)

    def stage_d(j):
        if j == 0:
            w1_cp.wait()
            w2_cp.wait()
        for r in range(NY):
            arrived(j, 1, r)
        psend[j] = mlp(grp[j, pl.ds(half, half)]).astype(BF16)
        swap(j).start()
        part[j % NPART] = mlp(grp[j, pl.ds(0, half)])

    rc, rd = 3 - 2 * c, 1 + 2 * c

    def q_far(j):
        return remote(qs.at[j, 0], rq.at[j, 0], qsem_s.at[j, 0], qsem_r.at[j, 0], ahead)

    def q_on(j):
        return remote(qs.at[j, 1], rq.at[j, 1], qsem_s.at[j, 1], qsem_r.at[j, 1], ahead)

    def q_near(j):
        return remote(qs.at[j, 2], rq.at[j, 2], qsem_s.at[j, 2], qsem_r.at[j, 2], behind)

    def q_wait(j, i):
        view = rq.at[j, i]
        pltpu.make_async_copy(view, view, qsem_r.at[j, i]).wait()

    def rows_of(r):
        return pl.ds(pl.multiple_of(r * ROWS, ROWS), ROWS)

    def pair_sum(j, r):
        return part[j % NPART, rows_of(r)] + precv[j, rows_of(r)].astype(F32)

    def stage_e(j):
        view = precv.at[j]
        pltpu.make_async_copy(view, view, psem_r.at[j]).wait()
        qs[j, 0] = pair_sum(j, 2).astype(BF16)
        q_far(j).start()
        qs[j, 2] = pair_sum(j, rd).astype(BF16)
        q_near(j).start()

    def stage_f(j):
        q_wait(j, 0)
        qs[j, 1] = (pair_sum(j, rc) + rq[j, 0].astype(F32)).astype(BF16)
        q_on(j).start()

    def give_back(k):
        dz, dx = OFFS[k]
        return pltpu.make_async_remote_copy(
            src_ref=ret.at[k],
            dst_ref=back.at[k],
            send_sem=rsend,
            recv_sem=rrecv.at[k // PER],
            device_id=to(NZ - dz, NX - dx),
            device_id_type=MESH,
        )

    own_out = pltpu.make_async_copy(ret.at[last], back.at[last], lsem.at[4])

    def stage_g(j):
        q_wait(j, 2)
        total = pair_sum(j, 0) + rq[j, 2].astype(F32)
        q_wait(j, 1)
        total = total + rq[j, 1].astype(F32)
        scaled = total * gates[j][:, :1]
        ret[pl.ds(j * PER, PER)] = scaled.reshape(PER, CAP, d_model).astype(BF16)
        for k in range(j * PER, j * PER + n_remote(j)):
            give_back(k).start()
        if j == NCH - 1:
            own_out.start()

    stages = dict(
        a=stage_a, b=stage_b, c=stage_c, d=stage_d, e=stage_e, f=stage_f, g=stage_g
    )
    for _, name, j in sorted((j + LAGS[n], n, j) for n in stages for j in range(NCH)):
        stages[name](j)

    acc = tok[...].astype(F32)
    for j in range(NCH):
        all_of(back, j * PER, n_remote(j), rrecv.at[j]).wait()
        if j == NCH - 1:
            own_out.wait()
        rows = back[pl.ds(j * PER, PER)].astype(F32).reshape(ROWS, d_model).astype(BF16)
        choose = jnp.where(
            lax.broadcasted_iota(jnp.int32, (n_tok, ROWS), 1) + j * ROWS == row_c, 1.0, 0.0
        ).astype(BF16)
        acc = acc + jnp.dot(choose, rows, preferred_element_type=F32)
    out_ref[...] = acc.astype(BF16)

    all_of(snd, 0, last, dsend).wait()
    all_of(ret, 0, last, rsend).wait()
    for j in range(NCH):
        ag_ahead(j).wait_send()
        ag_behind(j).wait_send()
        ag_on(j).wait_send()
        for r in range(NY):
            ag_side(j, r).wait_send()
        swap(j).wait_send()
        q_far(j).wait_send()
        q_on(j).wait_send()
        q_near(j).wait_send()


def body(tokens, assignment, centroids, norm_gain, inner_weight, outer_weight):
    n_tok, d = tokens.shape
    hidden = inner_weight.shape[1]
    half = NY * ROWS
    vmem, anyspace = pltpu.VMEM, pl.ANY
    dma = pltpu.SemaphoreType.DMA
    return pl.pallas_call(
        kernel,
        out_shape=jax.ShapeDtypeStruct((n_tok, d), BF16),
        in_specs=[
            pl.BlockSpec(memory_space=anyspace),
            pl.BlockSpec(memory_space=vmem),
            pl.BlockSpec(memory_space=vmem),
            pl.BlockSpec(memory_space=vmem),
            pl.BlockSpec(memory_space=anyspace),
            pl.BlockSpec(memory_space=anyspace),
        ],
        out_specs=pl.BlockSpec(memory_space=vmem),
        scratch_shapes=[
            vmem((n_tok, d), BF16),
            vmem((hidden, d), BF16),
            vmem((hidden, d), BF16),
            vmem((NCH * PER, CAP, d), BF16),
            vmem((NCH * PER, CAP, d), BF16),
            vmem((NCH, 2 * half, d), BF16),
            vmem((NCH, half, d), BF16),
            vmem((NCH, half, d), BF16),
            vmem((NPART, half, d), F32),
            vmem((NCH, 3, ROWS, d), BF16),
            vmem((NCH, 3, ROWS, d), BF16),
            vmem((NCH * PER, CAP, d), BF16),
            vmem((NCH * PER, CAP, d), BF16),
            vmem((NCH, ROWS, 128), F32),
            dma((5,)),
            dma,
            dma((NCH,)),
            dma((NCH, 8)),
            dma((NCH, 8)),
            dma((NCH,)),
            dma((NCH,)),
            dma((NCH, 3)),
            dma((NCH, 3)),
            dma,
            dma((NCH,)),
        ],
        compiler_params=pltpu.CompilerParams(
            collective_id=0, has_side_effects=True, vmem_limit_bytes=60 * 2**20
        ),
    )(tokens, assignment.reshape(1, n_tok), centroids, norm_gain, inner_weight, outer_weight)


def solution(mesh):
    in_specs = (
        P(("dp", "expert"), None),
        P(("dp", "expert")),
        P("expert", None),
        P("expert", None),
        P("expert", "dp", None),
        P("expert", "dp", None),
    )
    out_specs = P(("dp", "expert"), None)
    return jax.shard_map(body, mesh=mesh, in_specs=in_specs, out_specs=out_specs, check_vma=False)
```

```python
import functools

import jax
import jax.numpy as jnp
from jax import lax
from jax.experimental import pallas as pl
from jax.experimental.pallas import tpu as pltpu
from jax.sharding import PartitionSpec as P

MESH = pl.DeviceIdType.MESH
EPS = 1e-05
NZ, NX, NY = 16, 4, 4
CAP = 4
CHUNKS = ((1, 15), (4, 12), (7, 9), (3, 13), (8, 0), (5, 11), (6, 10), (2, 14))
NCH = len(CHUNKS)
PER = NX * len(CHUNKS[0])
LAGS = dict(a=0.0, b=0.9, c=1.6, d=2.3, e=3.2, f=4.0, g=4.9)
NPART = 5
XS = (1, 2, 3, 0)
OFFS = tuple((dz, dx) for c in CHUNKS for dz in c for dx in XS)
OWN = OFFS.index((0, 0))
ROWS = PER * CAP
F32, BF16 = jnp.float32, jnp.bfloat16


def kernel(
    tok_hbm, asg_ref, cen_ref, gain_ref, w1_hbm, w2_hbm, out_ref,
    tok, w1, w2, snd, rcv, grp, psend, precv, part, qs, rq, ret, back, gates,
    lsem, dsend, drecv, asend, arecv, psem_s, psem_r, qsem_s, qsem_r, rsend, rrecv,
):
    dp, e = lax.axis_index("dp"), lax.axis_index("expert")
    y, c = dp // 2, lax.rem(dp, 2)
    z, x = e // NX, lax.rem(e, NX)
    d_model = tok.shape[1]

    tok_cp = pltpu.make_async_copy(tok_hbm, tok, lsem.at[0])
    w1_cp = pltpu.make_async_copy(w1_hbm.at[0], w1, lsem.at[1])
    w2_cp = pltpu.make_async_copy(w2_hbm.at[0], w2, lsem.at[2])
    tok_cp.start()
    w1_cp.start()
    w2_cp.start()

    def chip(step):
        return lax.rem(y + step, NY) * 2 + c

    partner = (y * 2 + (1 - c), e)
    dirf = 1 + 2 * c
    dirb = 3 - 2 * c
    ahead, behind = (chip(dirf), e), (chip(dirb), e)

    def to(dz, dx):
        return (dp, lax.rem(z + dz, NZ) * NX + lax.rem(x + dx, NX))

    bar = pltpu.get_barrier_semaphore()
    peers = [to(*o) for o in OFFS if o != (0, 0)] + [partner, ahead, behind]
    for peer in peers:
        pl.semaphore_signal(bar, inc=1, device_id=peer, device_id_type=MESH)

    n_tok = tok.shape[0]
    a_row = asg_ref[...]
    ri = lax.broadcasted_iota(jnp.int32, (n_tok, n_tok), 0)
    ci = lax.broadcasted_iota(jnp.int32, (n_tok, n_tok), 1)
    a_lane = jnp.broadcast_to(a_row, (n_tok, n_tok))
    a_col = jnp.sum(jnp.where(ri == ci, a_lane, 0), axis=1, keepdims=True)
    same = a_lane == a_col
    pos_row = jnp.sum(jnp.where(same & (ri < ci), 1, 0), axis=0, keepdims=True)
    pos_col = jnp.sum(jnp.where(same & (ci < ri), 1, 0), axis=1, keepdims=True)

    def row_of(a, pos):
        dz = (a // NX - z + NZ) & (NZ - 1)
        dx = (a - z * NX - x + NZ * NX) & (NX - 1)
        kz = jnp.zeros_like(a)
        for i, v in enumerate(v for ch in CHUNKS for v in ch):
            kz = jnp.where(dz == v, i, kz)
        kx = (dx + NX - 1) & (NX - 1)
        return (kz * NX + kx) * CAP + pos


    row_r = row_of(a_row, pos_row)
    row_c = row_of(a_col, pos_col)
    n_slot = NCH * ROWS
    pick = jnp.where(
        lax.broadcasted_iota(jnp.int32, (n_slot, n_tok), 0) == row_r, 1.0, 0.0
    ).astype(BF16)
    tok_cp.wait()
    slots = jnp.dot(pick, tok[...], preferred_element_type=F32)
    snd[...] = slots.reshape(NCH * PER, CAP, d_model).astype(BF16)

    pl.semaphore_wait(bar, len(peers))

    def dispatch(k):
        return pltpu.make_async_remote_copy(
            src_ref=snd.at[k],
            dst_ref=rcv.at[k],
            send_sem=dsend,
            recv_sem=drecv.at[k // PER],
            device_id=to(*OFFS[k]),
            device_id_type=MESH,
        )

    remotes = NCH * PER - 1
    for k in range(NCH * PER):
        if k != OWN:
            dispatch(k).start()
    own_in = pltpu.make_async_copy(snd.at[OWN], rcv.at[OWN], lsem.at[3])
    own_in.start()

    def all_of(ref, first, count, sem):
        view = ref.at[pl.ds(first, count)]
        return pltpu.make_async_copy(view, view, sem)

    def n_remote(j):
        return PER - 1 if j == OWN // PER else PER

    def block(j, s, r):
        return grp.at[j, pl.ds((s * NY + r) * ROWS, ROWS)]

    def remote(src, dst, ssem, rsem, dev):
        return pltpu.make_async_remote_copy(
            src_ref=src, dst_ref=dst, send_sem=ssem, recv_sem=rsem,
            device_id=dev, device_id_type=MESH,
        )

    rf, rb = 1 + 2 * c, 3 - 2 * c

    def ag_ahead(j):
        return remote(block(j, 0, 0), block(j, 0, rf), asend.at[j, 0], arecv.at[j, rf], ahead)

    def ag_behind(j):
        return remote(block(j, 0, 0), block(j, 0, rb), asend.at[j, 1], arecv.at[j, rb], behind)

    def ag_on(j):
        return remote(block(j, 0, rf), block(j, 0, 2), asend.at[j, 2], arecv.at[j, 2], ahead)

    def ag_side(j, r):
        return remote(
            block(j, 0, r), block(j, 1, r), asend.at[j, 4 + r], arecv.at[j, NY + r], partner
        )

    def arrived(j, s, r):
        view = block(j, s, r)
        pltpu.make_async_copy(view, view, arecv.at[j, s * NY + r]).wait()

    def stage_a(j):
        all_of(rcv, j * PER, n_remote(j), drecv.at[j]).wait()
        if j == OWN // PER:
            own_in.wait()
        v = rcv[pl.ds(j * PER, PER)].astype(F32).reshape(ROWS, d_model)
        center = jnp.mean(v, axis=1, keepdims=True)
        dev = v - center
        spread = jnp.mean(dev * dev, axis=1, keepdims=True)
        normed = (dev * lax.rsqrt(spread + EPS) * gain_ref[...]).astype(BF16)
        grp[j, pl.ds(0, ROWS)] = normed
        ag_ahead(j).start()
        ag_behind(j).start()
        ag_side(j, 0).start()
        score = jnp.sum(v * cen_ref[...].astype(F32), axis=1, keepdims=True)
        gate = (1.0 / (1.0 + jnp.exp(-score))).astype(BF16).astype(F32)
        gates[j] = jnp.broadcast_to(gate, (ROWS, 128))

    def stage_b(j):
        arrived(j, 0, rf)
        ag_on(j).start()
        arrived(j, 0, rb)
        ag_side(j, 1).start()
        ag_side(j, 3).start()

    def stage_c(j):
        arrived(j, 0, 2)
        ag_side(j, 2).start()

    def mlp(rows):
        act = lax.dot_general(
            rows, w1[...], (((1,), (1,)), ((), ())), preferred_element_type=F32
        )
        hidden = jnp.maximum(act, 0.0).astype(BF16)
        return jnp.dot(hidden, w2[...], preferred_element_type=F32)

    half = NY * ROWS

    def swap(j):
        return remote(psend.at[j], precv.at[j], psem_s.at[j], psem_r.at[j], partner)

    def stage_d(j):
        if j == 0:
            w1_cp.wait()
            w2_cp.wait()
        for r in range(NY):
            arrived(j, 1, r)
        both = mlp(grp[j])
        psend[j] = both[half:].astype(BF16)
        swap(j).start()
        part[j % NPART] = both[:half]

    rc, rd = 3 - 2 * c, 1 + 2 * c

    def q_far(j):
        return remote(qs.at[j, 0], rq.at[j, 0], qsem_s.at[j, 0], qsem_r.at[j, 0], ahead)

    def q_on(j):
        return remote(qs.at[j, 1], rq.at[j, 1], qsem_s.at[j, 1], qsem_r.at[j, 1], ahead)

    def q_near(j):
        return remote(qs.at[j, 2], rq.at[j, 2], qsem_s.at[j, 2], qsem_r.at[j, 2], behind)

    def q_wait(j, i):
        view = rq.at[j, i]
        pltpu.make_async_copy(view, view, qsem_r.at[j, i]).wait()

    def rows_of(r):
        return pl.ds(pl.multiple_of(r * ROWS, ROWS), ROWS)

    def pair_sum(j, r):
        return part[j % NPART, rows_of(r)] + precv[j, rows_of(r)].astype(F32)

    def stage_e(j):
        view = precv.at[j]
        pltpu.make_async_copy(view, view, psem_r.at[j]).wait()
        qs[j, 0] = pair_sum(j, 2).astype(BF16)
        q_far(j).start()
        qs[j, 2] = pair_sum(j, rd).astype(BF16)
        q_near(j).start()

    def stage_f(j):
        q_wait(j, 0)
        qs[j, 1] = (pair_sum(j, rc) + rq[j, 0].astype(F32)).astype(BF16)
        q_on(j).start()

    def give_back(k):
        dz, dx = OFFS[k]
        return pltpu.make_async_remote_copy(
            src_ref=ret.at[k],
            dst_ref=back.at[k],
            send_sem=rsend,
            recv_sem=rrecv.at[k // PER],
            device_id=to(NZ - dz, NX - dx),
            device_id_type=MESH,
        )

    own_out = pltpu.make_async_copy(ret.at[OWN], back.at[OWN], lsem.at[4])

    def stage_g(j):
        q_wait(j, 2)
        total = pair_sum(j, 0) + rq[j, 2].astype(F32)
        q_wait(j, 1)
        total = total + rq[j, 1].astype(F32)
        scaled = total * gates[j][:, :1]
        ret[pl.ds(j * PER, PER)] = scaled.reshape(PER, CAP, d_model).astype(BF16)
        for k in range(j * PER, j * PER + n_remote(j)):
            give_back(k).start()
        if j == OWN // PER:
            own_out.start()

    stages = dict(
        a=stage_a, b=stage_b, c=stage_c, d=stage_d, e=stage_e, f=stage_f, g=stage_g
    )
    for _, name, j in sorted((j + LAGS[n], n, j) for n in stages for j in range(NCH)):
        stages[name](j)

    acc = tok[...].astype(F32)
    for j in range(NCH):
        all_of(back, j * PER, n_remote(j), rrecv.at[j]).wait()
        if j == OWN // PER:
            own_out.wait()
        rows = back[pl.ds(j * PER, PER)].astype(F32).reshape(ROWS, d_model).astype(BF16)
        choose = jnp.where(
            lax.broadcasted_iota(jnp.int32, (n_tok, ROWS), 1) + j * ROWS == row_c, 1.0, 0.0
        ).astype(BF16)
        acc = acc + jnp.dot(choose, rows, preferred_element_type=F32)
    out_ref[...] = acc.astype(BF16)

    all_of(snd, 0, remotes, dsend).wait()
    all_of(ret, 0, remotes, rsend).wait()
    for j in range(NCH):
        ag_ahead(j).wait_send()
        ag_behind(j).wait_send()
        ag_on(j).wait_send()
        for r in range(NY):
            ag_side(j, r).wait_send()
        swap(j).wait_send()
        q_far(j).wait_send()
        q_on(j).wait_send()
        q_near(j).wait_send()


def body(tokens, assignment, centroids, norm_gain, inner_weight, outer_weight):
    n_tok, d = tokens.shape
    hidden = inner_weight.shape[1]
    half = NY * ROWS
    vmem, anyspace = pltpu.VMEM, pl.ANY
    dma = pltpu.SemaphoreType.DMA
    return pl.pallas_call(
        kernel,
        out_shape=jax.ShapeDtypeStruct((n_tok, d), BF16),
        in_specs=[
            pl.BlockSpec(memory_space=anyspace),
            pl.BlockSpec(memory_space=vmem),
            pl.BlockSpec(memory_space=vmem),
            pl.BlockSpec(memory_space=vmem),
            pl.BlockSpec(memory_space=anyspace),
            pl.BlockSpec(memory_space=anyspace),
        ],
        out_specs=pl.BlockSpec(memory_space=vmem),
        scratch_shapes=[
            vmem((n_tok, d), BF16),
            vmem((hidden, d), BF16),
            vmem((hidden, d), BF16),
            vmem((NCH * PER, CAP, d), BF16),
            vmem((NCH * PER, CAP, d), BF16),
            vmem((NCH, 2 * half, d), BF16),
            vmem((NCH, half, d), BF16),
            vmem((NCH, half, d), BF16),
            vmem((NPART, half, d), F32),
            vmem((NCH, 3, ROWS, d), BF16),
            vmem((NCH, 3, ROWS, d), BF16),
            vmem((NCH * PER, CAP, d), BF16),
            vmem((NCH * PER, CAP, d), BF16),
            vmem((NCH, ROWS, 128), F32),
            dma((5,)),
            dma,
            dma((NCH,)),
            dma((NCH, 8)),
            dma((NCH, 8)),
            dma((NCH,)),
            dma((NCH,)),
            dma((NCH, 3)),
            dma((NCH, 3)),
            dma,
            dma((NCH,)),
        ],
        compiler_params=pltpu.CompilerParams(
            collective_id=0, has_side_effects=True, vmem_limit_bytes=60 * 2**20
        ),
    )(tokens, assignment.reshape(1, n_tok), centroids, norm_gain, inner_weight, outer_weight)


def solution(mesh):
    in_specs = (
        P(("dp", "expert"), None),
        P(("dp", "expert")),
        P("expert", None),
        P("expert", None),
        P("expert", "dp", None),
        P("expert", "dp", None),
    )
    out_specs = P(("dp", "expert"), None)
    return jax.shard_map(body, mesh=mesh, in_specs=in_specs, out_specs=out_specs, check_vma=False)
```

```python
import functools

import jax
import jax.numpy as jnp
from jax import lax
from jax.experimental import pallas as pl
from jax.experimental.pallas import tpu as pltpu
from jax.sharding import PartitionSpec as P

MESH = pl.DeviceIdType.MESH
EPS = 1e-05
NZ, NX, NY = 16, 4, 4
CAP = 4
CHUNKS = ((1, 15), (4, 12), (7, 9), (5, 11), (8, 0), (6, 10), (3, 13), (2, 14))
NCH = len(CHUNKS)
PER = NX * len(CHUNKS[0])
LAGS = dict(a=0.0, b=0.9, c=1.6, d=2.3, e=3.2, f=4.0, g=4.9)
NPART = 5
XS = (1, 2, 3, 0)
OFFS = tuple((dz, dx) for c in CHUNKS for dz in c for dx in XS)
OWN = OFFS.index((0, 0))
ROWS = PER * CAP
F32, BF16 = jnp.float32, jnp.bfloat16


def kernel(
    tok_hbm, asg_ref, cen_ref, gain_ref, w1_hbm, w2_hbm, out_ref,
    tok, w1, w2, snd, rcv, grp, psend, precv, part, qs, rq, ret, back, gates,
    lsem, dsend, drecv, asend, arecv, psem_s, psem_r, qsem_s, qsem_r, rsend, rrecv,
):
    dp, e = lax.axis_index("dp"), lax.axis_index("expert")
    y, c = dp // 2, lax.rem(dp, 2)
    z, x = e // NX, lax.rem(e, NX)
    d_model = tok.shape[1]

    tok_cp = pltpu.make_async_copy(tok_hbm, tok, lsem.at[0])
    w1_cp = pltpu.make_async_copy(w1_hbm.at[0], w1, lsem.at[1])
    w2_cp = pltpu.make_async_copy(w2_hbm.at[0], w2, lsem.at[2])
    tok_cp.start()
    w1_cp.start()
    w2_cp.start()

    def chip(step):
        return lax.rem(y + step, NY) * 2 + c

    partner = (y * 2 + (1 - c), e)
    dirf = 1 + 2 * c
    dirb = 3 - 2 * c
    ahead, behind = (chip(dirf), e), (chip(dirb), e)

    def to(dz, dx):
        return (dp, lax.rem(z + dz, NZ) * NX + lax.rem(x + dx, NX))

    bar = pltpu.get_barrier_semaphore()
    peers = [to(*o) for o in OFFS if o != (0, 0)] + [partner, ahead, behind]
    for peer in peers:
        pl.semaphore_signal(bar, inc=1, device_id=peer, device_id_type=MESH)

    n_tok = tok.shape[0]
    a_row = asg_ref[...]
    ri = lax.broadcasted_iota(jnp.int32, (n_tok, n_tok), 0)
    ci = lax.broadcasted_iota(jnp.int32, (n_tok, n_tok), 1)
    a_lane = jnp.broadcast_to(a_row, (n_tok, n_tok))
    a_col = jnp.sum(jnp.where(ri == ci, a_lane, 0), axis=1, keepdims=True)
    same = a_lane == a_col
    pos_row = jnp.sum(jnp.where(same & (ri < ci), 1, 0), axis=0, keepdims=True)
    pos_col = jnp.sum(jnp.where(same & (ci < ri), 1, 0), axis=1, keepdims=True)

    def row_of(a, pos):
        dz = (a // NX - z + NZ) & (NZ - 1)
        dx = (a - z * NX - x + NZ * NX) & (NX - 1)
        kz = jnp.zeros_like(a)
        for i, v in enumerate(v for ch in CHUNKS for v in ch):
            kz = jnp.where(dz == v, i, kz)
        kx = (dx + NX - 1) & (NX - 1)
        return (kz * NX + kx) * CAP + pos


    row_r = row_of(a_row, pos_row)
    row_c = row_of(a_col, pos_col)
    n_slot = NCH * ROWS
    pick = jnp.where(
        lax.broadcasted_iota(jnp.int32, (n_slot, n_tok), 0) == row_r, 1.0, 0.0
    ).astype(BF16)
    tok_cp.wait()
    slots = jnp.dot(pick, tok[...], preferred_element_type=F32)
    snd[...] = slots.reshape(NCH * PER, CAP, d_model).astype(BF16)

    pl.semaphore_wait(bar, len(peers))

    def dispatch(k):
        return pltpu.make_async_remote_copy(
            src_ref=snd.at[k],
            dst_ref=rcv.at[k],
            send_sem=dsend,
            recv_sem=drecv.at[k // PER],
            device_id=to(*OFFS[k]),
            device_id_type=MESH,
        )

    remotes = NCH * PER - 1
    for k in range(NCH * PER):
        if k != OWN:
            dispatch(k).start()
    own_in = pltpu.make_async_copy(snd.at[OWN], rcv.at[OWN], lsem.at[3])
    own_in.start()

    def all_of(ref, first, count, sem):
        view = ref.at[pl.ds(first, count)]
        return pltpu.make_async_copy(view, view, sem)

    def n_remote(j):
        return PER - 1 if j == OWN // PER else PER

    def block(j, s, r):
        return grp.at[j, pl.ds((s * NY + r) * ROWS, ROWS)]

    def remote(src, dst, ssem, rsem, dev):
        return pltpu.make_async_remote_copy(
            src_ref=src, dst_ref=dst, send_sem=ssem, recv_sem=rsem,
            device_id=dev, device_id_type=MESH,
        )

    rf, rb = 1 + 2 * c, 3 - 2 * c

    def ag_ahead(j):
        return remote(block(j, 0, 0), block(j, 0, rf), asend.at[j, 0], arecv.at[j, rf], ahead)

    def ag_behind(j):
        return remote(block(j, 0, 0), block(j, 0, rb), asend.at[j, 1], arecv.at[j, rb], behind)

    def ag_on(j):
        return remote(block(j, 0, rf), block(j, 0, 2), asend.at[j, 2], arecv.at[j, 2], ahead)

    def ag_side(j, r):
        return remote(
            block(j, 0, r), block(j, 1, r), asend.at[j, 4 + r], arecv.at[j, NY + r], partner
        )

    def arrived(j, s, r):
        view = block(j, s, r)
        pltpu.make_async_copy(view, view, arecv.at[j, s * NY + r]).wait()

    def stage_a(j):
        all_of(rcv, j * PER, n_remote(j), drecv.at[j]).wait()
        if j == OWN // PER:
            own_in.wait()
        v = rcv[pl.ds(j * PER, PER)].astype(F32).reshape(ROWS, d_model)
        center = jnp.mean(v, axis=1, keepdims=True)
        dev = v - center
        spread = jnp.mean(dev * dev, axis=1, keepdims=True)
        normed = (dev * lax.rsqrt(spread + EPS) * gain_ref[...]).astype(BF16)
        grp[j, pl.ds(0, ROWS)] = normed
        ag_ahead(j).start()
        ag_behind(j).start()
        ag_side(j, 0).start()
        score = jnp.sum(v * cen_ref[...].astype(F32), axis=1, keepdims=True)
        gate = (1.0 / (1.0 + jnp.exp(-score))).astype(BF16).astype(F32)
        gates[j] = jnp.broadcast_to(gate, (ROWS, 128))

    def stage_b(j):
        arrived(j, 0, rf)
        ag_on(j).start()
        arrived(j, 0, rb)
        ag_side(j, 1).start()
        ag_side(j, 3).start()

    def stage_c(j):
        arrived(j, 0, 2)
        ag_side(j, 2).start()

    def mlp(rows):
        act = lax.dot_general(
            rows, w1[...], (((1,), (1,)), ((), ())), preferred_element_type=F32
        )
        hidden = jnp.maximum(act, 0.0).astype(BF16)
        return jnp.dot(hidden, w2[...], preferred_element_type=F32)

    half = NY * ROWS

    def swap(j):
        return remote(psend.at[j], precv.at[j], psem_s.at[j], psem_r.at[j], partner)

    def stage_d(j):
        if j == 0:
            w1_cp.wait()
            w2_cp.wait()
        for r in range(NY):
            arrived(j, 1, r)
        both = mlp(grp[j])
        psend[j] = both[half:].astype(BF16)
        swap(j).start()
        part[j % NPART] = both[:half]

    rc, rd = 3 - 2 * c, 1 + 2 * c

    def q_far(j):
        return remote(qs.at[j, 0], rq.at[j, 0], qsem_s.at[j, 0], qsem_r.at[j, 0], ahead)

    def q_on(j):
        return remote(qs.at[j, 1], rq.at[j, 1], qsem_s.at[j, 1], qsem_r.at[j, 1], ahead)

    def q_near(j):
        return remote(qs.at[j, 2], rq.at[j, 2], qsem_s.at[j, 2], qsem_r.at[j, 2], behind)

    def q_wait(j, i):
        view = rq.at[j, i]
        pltpu.make_async_copy(view, view, qsem_r.at[j, i]).wait()

    def rows_of(r):
        return pl.ds(pl.multiple_of(r * ROWS, ROWS), ROWS)

    def pair_sum(j, r):
        return part[j % NPART, rows_of(r)] + precv[j, rows_of(r)].astype(F32)

    def stage_e(j):
        view = precv.at[j]
        pltpu.make_async_copy(view, view, psem_r.at[j]).wait()
        qs[j, 0] = pair_sum(j, 2).astype(BF16)
        q_far(j).start()
        qs[j, 2] = pair_sum(j, rd).astype(BF16)
        q_near(j).start()

    def stage_f(j):
        q_wait(j, 0)
        qs[j, 1] = (pair_sum(j, rc) + rq[j, 0].astype(F32)).astype(BF16)
        q_on(j).start()

    def give_back(k):
        dz, dx = OFFS[k]
        return pltpu.make_async_remote_copy(
            src_ref=ret.at[k],
            dst_ref=back.at[k],
            send_sem=rsend,
            recv_sem=rrecv.at[k // PER],
            device_id=to(NZ - dz, NX - dx),
            device_id_type=MESH,
        )

    own_out = pltpu.make_async_copy(ret.at[OWN], back.at[OWN], lsem.at[4])

    def stage_g(j):
        q_wait(j, 2)
        total = pair_sum(j, 0) + rq[j, 2].astype(F32)
        q_wait(j, 1)
        total = total + rq[j, 1].astype(F32)
        scaled = total * gates[j][:, :1]
        ret[pl.ds(j * PER, PER)] = scaled.reshape(PER, CAP, d_model).astype(BF16)
        for k in range(j * PER, j * PER + n_remote(j)):
            give_back(k).start()
        if j == OWN // PER:
            own_out.start()

    stages = dict(
        a=stage_a, b=stage_b, c=stage_c, d=stage_d, e=stage_e, f=stage_f, g=stage_g
    )
    for _, name, j in sorted((j + LAGS[n], n, j) for n in stages for j in range(NCH)):
        stages[name](j)

    acc = tok[...].astype(F32)
    for j in range(NCH):
        all_of(back, j * PER, n_remote(j), rrecv.at[j]).wait()
        if j == OWN // PER:
            own_out.wait()
        rows = back[pl.ds(j * PER, PER)].astype(F32).reshape(ROWS, d_model).astype(BF16)
        choose = jnp.where(
            lax.broadcasted_iota(jnp.int32, (n_tok, ROWS), 1) + j * ROWS == row_c, 1.0, 0.0
        ).astype(BF16)
        acc = acc + jnp.dot(choose, rows, preferred_element_type=F32)
    out_ref[...] = acc.astype(BF16)

    all_of(snd, 0, remotes, dsend).wait()
    all_of(ret, 0, remotes, rsend).wait()
    for j in range(NCH):
        ag_ahead(j).wait_send()
        ag_behind(j).wait_send()
        ag_on(j).wait_send()
        for r in range(NY):
            ag_side(j, r).wait_send()
        swap(j).wait_send()
        q_far(j).wait_send()
        q_on(j).wait_send()
        q_near(j).wait_send()


def body(tokens, assignment, centroids, norm_gain, inner_weight, outer_weight):
    n_tok, d = tokens.shape
    hidden = inner_weight.shape[1]
    half = NY * ROWS
    vmem, anyspace = pltpu.VMEM, pl.ANY
    dma = pltpu.SemaphoreType.DMA
    return pl.pallas_call(
        kernel,
        out_shape=jax.ShapeDtypeStruct((n_tok, d), BF16),
        in_specs=[
            pl.BlockSpec(memory_space=anyspace),
            pl.BlockSpec(memory_space=vmem),
            pl.BlockSpec(memory_space=vmem),
            pl.BlockSpec(memory_space=vmem),
            pl.BlockSpec(memory_space=anyspace),
            pl.BlockSpec(memory_space=anyspace),
        ],
        out_specs=pl.BlockSpec(memory_space=vmem),
        scratch_shapes=[
            vmem((n_tok, d), BF16),
            vmem((hidden, d), BF16),
            vmem((hidden, d), BF16),
            vmem((NCH * PER, CAP, d), BF16),
            vmem((NCH * PER, CAP, d), BF16),
            vmem((NCH, 2 * half, d), BF16),
            vmem((NCH, half, d), BF16),
            vmem((NCH, half, d), BF16),
            vmem((NPART, half, d), F32),
            vmem((NCH, 3, ROWS, d), BF16),
            vmem((NCH, 3, ROWS, d), BF16),
            vmem((NCH * PER, CAP, d), BF16),
            vmem((NCH * PER, CAP, d), BF16),
            vmem((NCH, ROWS, 128), F32),
            dma((5,)),
            dma,
            dma((NCH,)),
            dma((NCH, 8)),
            dma((NCH, 8)),
            dma((NCH,)),
            dma((NCH,)),
            dma((NCH, 3)),
            dma((NCH, 3)),
            dma,
            dma((NCH,)),
        ],
        compiler_params=pltpu.CompilerParams(
            collective_id=0, has_side_effects=True, vmem_limit_bytes=60 * 2**20
        ),
    )(tokens, assignment.reshape(1, n_tok), centroids, norm_gain, inner_weight, outer_weight)


def solution(mesh):
    in_specs = (
        P(("dp", "expert"), None),
        P(("dp", "expert")),
        P("expert", None),
        P("expert", None),
        P("expert", "dp", None),
        P("expert", "dp", None),
    )
    out_specs = P(("dp", "expert"), None)
    return jax.shard_map(body, mesh=mesh, in_specs=in_specs, out_specs=out_specs, check_vma=False)
```
